8 devices in a mesh: dp: 1 (over z), tp: 2 (over y), ep: 4 (over x, core).
Axes of the slice: x: 2, y: 2, z: 1, core: 2. Of those that a mesh axis runs over, the one named last changes fastest.
Arguments:
- tokens: bfloat16 [16384, 2048], P(('dp', 'ep'))
- expert_ids: int32 [16384, 2], P(('dp', 'ep'))
- norm_gain: bfloat16 [2048], replicated
- router_w: bfloat16 [2048, 8], replicated
- w_gate: bfloat16 [8, 2048, 5632], P('ep', None, 'tp')
- w_up: bfloat16 [8, 2048, 5632], P('ep', None, 'tp')
- w_down: bfloat16 [8, 5632, 2048], P('ep', 'tp')
Outputs:
- output: bfloat16 [16384, 2048], P(('dp', 'ep'))
All inputs are finite; a program needn't handle non-finite values.
Results may differ from the reference program's by a relative error of at most 0.012134.
Values are sent between devices in bfloat16 or wider.
A program may use at most 1 GiB of HBM per device.

```python
import jax
import jax.numpy as jnp
from jax import lax

MODEL_DIM = 2048
FFN_DIM = 5632
NUM_EXPERTS = 8
TOP_K = 2
EP_SIZE = 4
TOK_DEV = 4096
TOKENS = EP_SIZE * TOK_DEV
SLOT_CAP = 2 * TOP_K * TOK_DEV // NUM_EXPERTS
EXPERT_CAP = EP_SIZE * SLOT_CAP
NORM_EPS = 1e-5


def route_block(key):
    mean_load = TOP_K * TOK_DEV // NUM_EXPERTS
    key_lift, key_perm, key_tok = jax.random.split(key, 3)
    lifts = jax.random.randint(key_lift, (NUM_EXPERTS,), 1, mean_load, jnp.int32)
    lifts = lifts.at[0].set(mean_load).at[1].set(0)
    loads = mean_load + lifts - jnp.roll(lifts, -1)
    order = jnp.repeat(jnp.arange(NUM_EXPERTS, dtype=jnp.int32), loads, total_repeat_length=TOP_K * TOK_DEV)
    choice = order.reshape(TOP_K, TOK_DEV).T
    relabel = jax.random.permutation(key_perm, NUM_EXPERTS).astype(jnp.int32)
    shuffle = jax.random.permutation(key_tok, TOK_DEV)
    return relabel[choice][shuffle]


def setup_inputs(seed: int = 0, part: int = 0) -> dict:
    keys = jax.random.split(jax.random.key(seed), 5)
    tok_key = jax.random.fold_in(jax.random.key(seed + 1), part)
    route_key = jax.random.fold_in(jax.random.key(seed + 2), part)
    tokens = jax.random.normal(tok_key, (TOKENS, MODEL_DIM), jnp.float32)
    expert_ids = jax.vmap(route_block)(jax.random.split(route_key, EP_SIZE)).reshape(TOKENS, TOP_K)
    norm_gain = 1.0 + 0.5 * jax.random.normal(keys[0], (MODEL_DIM,), jnp.float32)
    router_w = jax.random.normal(keys[1], (MODEL_DIM, NUM_EXPERTS), jnp.float32) * MODEL_DIM ** -0.5
    w_gate = jax.random.normal(keys[2], (NUM_EXPERTS, MODEL_DIM, FFN_DIM), jnp.float32) * MODEL_DIM ** -0.5
    w_up = jax.random.normal(keys[3], (NUM_EXPERTS, MODEL_DIM, FFN_DIM), jnp.float32) * MODEL_DIM ** -0.5
    w_down = jax.random.normal(keys[4], (NUM_EXPERTS, FFN_DIM, MODEL_DIM), jnp.float32) * (2.0 * FFN_DIM ** -0.5)
    return {'tokens': tokens.astype(jnp.bfloat16), 'expert_ids': expert_ids, 'norm_gain': norm_gain.astype(jnp.bfloat16), 'router_w': router_w.astype(jnp.bfloat16), 'w_gate': w_gate.astype(jnp.bfloat16), 'w_up': w_up.astype(jnp.bfloat16), 'w_down': w_down.astype(jnp.bfloat16)}


def expert_ffn(operands):
    rows, gate_mat, up_mat, down_mat = operands
    gate_act = jnp.dot(rows, gate_mat, preferred_element_type=jnp.float32)
    up_act = jnp.dot(rows, up_mat, preferred_element_type=jnp.float32)
    hidden = (jax.nn.silu(gate_act) * up_act).astype(jnp.bfloat16)
    return jnp.dot(hidden, down_mat, preferred_element_type=jnp.float32).astype(jnp.bfloat16)


def reference(tokens, expert_ids, norm_gain, router_w, w_gate, w_up, w_down):
    tok_f32 = tokens.astype(jnp.float32)
    inv_rms = lax.rsqrt(jnp.mean(tok_f32 * tok_f32, axis=-1, keepdims=True) + NORM_EPS)
    normed = (tok_f32 * inv_rms * norm_gain.astype(jnp.float32)).astype(jnp.bfloat16)
    logits = jnp.dot(normed, router_w, preferred_element_type=jnp.float32)
    gates = jax.nn.softmax(jnp.take_along_axis(logits, expert_ids, axis=1), axis=-1)
    flat_ids = expert_ids.reshape(-1)
    onehot = (flat_ids[:, None] == jnp.arange(NUM_EXPERTS, dtype=jnp.int32)[None, :]).astype(jnp.int32)
    slot_ids = jnp.sum(jnp.cumsum(onehot, axis=0) * onehot, axis=1) - 1
    row_tok = jnp.arange(TOKENS * TOP_K, dtype=jnp.int32) // TOP_K
    src_rows = jnp.zeros((NUM_EXPERTS, EXPERT_CAP), jnp.int32).at[flat_ids, slot_ids].set(row_tok)
    buffers = normed[src_rows]
    expert_out = lax.map(expert_ffn, (buffers, w_gate, w_up, w_down))
    picked = expert_out[flat_ids, slot_ids].reshape(TOKENS, TOP_K, MODEL_DIM).astype(jnp.float32)
    mixed = jnp.sum(gates[:, :, None] * picked, axis=1)
    return (tok_f32 + mixed).astype(jnp.bfloat16)
```

```python
import functools

import jax
import jax.numpy as jnp
from jax import lax
from jax.experimental import pallas as pl
from jax.experimental.pallas import tpu as pltpu
from jax.sharding import PartitionSpec as P

NORM_EPS = 1e-5
ALIGN = 16
PIECE = 512
SUB = 128
TILE = 512
FCH = 256
RP = 2560
ANY = pl.BlockSpec(memory_space=pl.ANY)
SMEM = pl.BlockSpec(memory_space=pltpu.SMEM)
VMEM = pl.BlockSpec(memory_space=pltpu.VMEM)
CHUNKS = ((0, 0, 4, 0, 1), (1, 0, 4, 0, 1)) + tuple((2, q, 2, 1, 0) for q in range(4))


TIERS = ((2112, 1056), (4224, 2112))


def count_at(cnt, block, exp, quarter, half):
    return cnt[((block * 8 + exp) * 4 + quarter) * 2 + half]


def padded(c):
    return (c + (ALIGN - 1)) // ALIGN * ALIGN


def half_rows(cnt, me, exp, chunk, half):
    rel, q0, n, dr, dq = CHUNKS[chunk]
    tot = jnp.int32(0)
    for a in range(n):
        tot += padded(count_at(cnt, me ^ (rel + a * dr), exp, q0 + a * dq, half))
    return tot


def ffn_kernel(chunk, pos_ref, cnt_ref, rank_ref, *refs):
    rel, q0, n, dr, dq = CHUNKS[chunk]
    toks, (w1, w3, w2, send, keep, tokb, hbuf, acc, b1, b3, b2, tsem, wsem, osem) = refs[:n], refs[n:]
    me, half = pos_ref[0], pos_ref[1]
    nf = w1.shape[2] // FCH
    ntok = 2 * PIECE

    def w_copies(g):
        e, f, s = g // nf, g % nf, g % 2
        cols = pl.ds(pl.multiple_of(f * FCH, FCH), FCH)
        return (pltpu.make_async_copy(w1.at[e, :, cols], b1.at[s], wsem.at[s, 0]),
                pltpu.make_async_copy(w3.at[e, :, cols], b3.at[s], wsem.at[s, 1]),
                pltpu.make_async_copy(w2.at[e, cols, :], b2.at[s], wsem.at[s, 2]))

    def tok_copy(a):
        return pltpu.make_async_copy(toks[a], tokb.at[pl.ds(a * ntok, ntok)], tsem.at[a])

    for a in range(n):
        tok_copy(a).start()
    for c in w_copies(0):
        c.start()
    for a in range(n):
        tok_copy(a).wait()

    def expert(e, bases):
        def piece(p, row):
            t, a = jnp.where(p < n, 1 - half, half), p % n
            r, q = rel + a * dr, q0 + a * dq
            c = count_at(cnt_ref, me ^ r, 2 * me + e, q, t)
            ranks = rank_ref[pl.ds(((r * 2 + e) * 4 + q) * 2 + t, 1), :]
            tok = pl.ds(pl.multiple_of(a * ntok + t * PIECE, PIECE), PIECE)

            def sub(s, _):
                rows = lax.broadcasted_iota(jnp.int32, (SUB, PIECE), 0) + s * SUB
                sel = jnp.where(rows == ranks, 1.0, 0.0).astype(jnp.bfloat16)
                got = jnp.dot(sel, tokb[tok, :], preferred_element_type=jnp.float32)
                hbuf[pl.ds(pl.multiple_of(row + s * SUB, ALIGN), SUB), :] = got.astype(jnp.bfloat16)
                return 0

            lax.fori_loop(0, (c + SUB - 1) // SUB, sub, 0)
            return row + padded(c)

        first = lax.fori_loop(0, n, piece, jnp.int32(0))
        total = lax.fori_loop(n, 2 * n, piece, first)
        half_tile = TILE // 2
        nt = (total + half_tile - 1) // TILE
        rest = total > nt * TILE

        def tile(j, rows=TILE):
            return pl.ds(pl.multiple_of(j * TILE, TILE), rows)

        def over_tiles(do):
            pl.loop(0, nt)(lambda j: do(tile(j)))
            pl.when(rest)(lambda: do(tile(nt, half_tile)))

        def clear(at):
            acc[at, :] = jnp.zeros((at.size, acc.shape[1]), jnp.float32)

        over_tiles(clear)

        def width(f, _):
            g = e * nf + f
            s = g % 2

            @pl.when(g + 1 < 2 * nf)
            def _():
                for c in w_copies(g + 1):
                    c.start()

            for c in w_copies(g):
                c.wait()

            def rows(at):
                h = hbuf[at, :]
                a = jnp.dot(h, b1[s], preferred_element_type=jnp.float32)
                b = jnp.dot(h, b3[s], preferred_element_type=jnp.float32)
                u = (jax.nn.silu(a) * b).astype(jnp.bfloat16)
                acc[at, :] += jnp.dot(u, b2[s], preferred_element_type=jnp.float32)

            over_tiles(rows)
            return 0

        lax.fori_loop(0, nf, width, 0)

        def cast(at):
            hbuf[at, :] = acc[at, :].astype(jnp.bfloat16)

        over_tiles(cast)
        ends = []
        for dst, base, lo, hi in ((send, bases[0], 0, first), (keep, bases[1], first, total)):
            size = hi - lo
            whole = size // SUB

            def copy(at, rows):
                return pltpu.make_async_copy(hbuf.at[pl.ds(pl.multiple_of(lo + at, ALIGN), rows)],
                                             dst.at[pl.ds(pl.multiple_of(base + at, ALIGN), rows)], osem)

            def big(j, wait):
                c = copy(j * SUB, SUB)
                c.wait() if wait else c.start()

            def small(j, wait):
                c = copy(whole * SUB + j * ALIGN, ALIGN)
                c.wait() if wait else c.start()

            for wait in (False, True):
                pl.loop(0, whole)(lambda j: big(j, wait))
                pl.loop(0, (size - whole * SUB) // ALIGN)(lambda j: small(j, wait))
            ends.append(base + size)
        return tuple(ends)

    lax.fori_loop(0, 2, expert, (jnp.int32(0), jnp.int32(0)))


def run_ffn(chunk, cap, pos, cnt, ranks, toks, w1, w3, w2):
    n = CHUNKS[chunk][2]
    dim = w1.shape[1]
    width = w1.shape[2]
    rows = 1024 * n // 2 + 128 * n
    return pl.pallas_call(
        functools.partial(ffn_kernel, chunk),
        out_shape=[jax.ShapeDtypeStruct((cap, dim), jnp.bfloat16)] * 2,
        in_specs=[SMEM, SMEM, VMEM] + [ANY] * (n + 3),
        out_specs=[ANY, ANY],
        scratch_shapes=[
            pltpu.VMEM((n * 2 * PIECE, dim), jnp.bfloat16),
            pltpu.VMEM((RP, dim), jnp.bfloat16),
            pltpu.VMEM((RP, dim), jnp.float32),
            pltpu.VMEM((2, dim, FCH), jnp.bfloat16),
            pltpu.VMEM((2, dim, FCH), jnp.bfloat16),
            pltpu.VMEM((2, FCH, dim), jnp.bfloat16),
            pltpu.SemaphoreType.DMA((n,)),
            pltpu.SemaphoreType.DMA((2, 3)),
            pltpu.SemaphoreType.DMA,
        ],
        compiler_params=pltpu.CompilerParams(vmem_limit_bytes=62 * 1024 * 1024),
        cost_estimate=pl.CostEstimate(flops=rows * 6 * dim * width, bytes_accessed=6 * dim * width * 2, transcendentals=0),
        name=f"ffn{chunk}",
    )(pos, cnt, ranks, *toks, w1, w3, w2)


def mix_kernel(quarter, pos_ref, cnt_ref, ranks, gates, tok, own, mate, far, far_mate, out, rb, sem):
    me, half = pos_ref[0], pos_ref[1]
    dim = out.shape[1]

    def source(r, e):
        peer = me ^ r
        chunk = r if r < 2 else 2 + quarter
        base = half_rows(cnt_ref, peer, 2 * peer, chunk, half) if e else jnp.int32(0)
        if r < 2:
            for q in range(quarter):
                base += padded(count_at(cnt_ref, me, 2 * peer + e, q, half))
        elif r == 3:
            base += padded(count_at(cnt_ref, me ^ 1, 2 * peer + e, quarter, half))
        return (own, mate, far, far_mate)[r], base

    pairs = [(r, e) for r in range(4) for e in range(2)]
    places = [source(r, e) for r, e in pairs]

    def rows_at(i, s):
        buf, base = places[i]
        return jnp.minimum(base + s * SUB, buf.shape[0] - SUB)

    def rows_copy(i, s, slot):
        buf = places[i][0]
        return pltpu.make_async_copy(buf.at[pl.ds(pl.multiple_of(rows_at(i, s), ALIGN), SUB)], rb.at[slot], sem.at[slot])

    rows_copy(0, 0, 0).start()
    rows_copy(1, 0, 1).start()
    out_f32 = tok[...].astype(jnp.float32)
    for i, (r, e) in enumerate(pairs):
        exp = 2 * (me ^ r) + e
        c = count_at(cnt_ref, me, exp, quarter, half)
        if i + 2 < len(pairs):
            rows_copy(i + 2, 0, (i + 2) % 3).start()
        lane = lax.broadcasted_iota(jnp.int32, ranks.shape, 1) == exp
        rank = jnp.sum(jnp.where(lane, ranks[...], 0), axis=1, keepdims=True)
        gate = jnp.sum(jnp.where(lane, gates[...], 0.0), axis=1, keepdims=True)

        def pick(s, slot):
            shift = rows_at(i, s) - places[i][1]
            row = lax.broadcasted_iota(jnp.int32, (SUB, dim), 0) + shift
            y = jnp.where((row >= s * SUB) & (row < c), rb[slot].astype(jnp.float32), 0.0).astype(jnp.bfloat16)
            col = lax.broadcasted_iota(jnp.int32, (PIECE, SUB), 1) + shift
            sel = jnp.where(col == rank, 1.0, 0.0).astype(jnp.bfloat16)
            return jnp.dot(sel, y, preferred_element_type=jnp.float32) * gate

        rows_copy(i, 0, i % 3).wait()
        out_f32 = out_f32 + pick(0, i % 3)

        def more(s, tot):
            cp = rows_copy(i, s, 3)
            cp.start()
            cp.wait()
            return tot + pick(s, 3)

        out_f32 = lax.fori_loop(1, (c + SUB - 1) // SUB, more, out_f32)
    out[...] = out_f32.astype(out.dtype)


def run_mix(quarter, pos, cnt, ranks, gates, tok, *rows):
    dim = tok.shape[1]
    return pl.pallas_call(
        functools.partial(mix_kernel, quarter),
        out_shape=jax.ShapeDtypeStruct(tok.shape, tok.dtype),
        in_specs=[SMEM, SMEM, VMEM, VMEM, VMEM] + [ANY] * 4,
        out_specs=VMEM,
        scratch_shapes=[pltpu.VMEM((4, SUB, dim), jnp.bfloat16), pltpu.SemaphoreType.DMA((4,))],
        cost_estimate=pl.CostEstimate(flops=12 * PIECE * SUB * dim * 2, bytes_accessed=12 * SUB * dim * 2, transcendentals=0),
        name=f"mix{quarter}",
    )(pos, cnt, ranks, gates, tok, *rows)


def tier_kernel(caps, cnt_ref, out):
    need = [jnp.int32(0), jnp.int32(0)]
    for k in range(len(CHUNKS)):
        kind = 0 if k < 2 else 1

        def device(i, m):
            me, half = i // 2, i % 2
            return jnp.maximum(m, half_rows(cnt_ref, me, 2 * me, k, half) + half_rows(cnt_ref, me, 2 * me + 1, k, half))

        need[kind] = lax.fori_loop(0, 8, device, need[kind])
    tier = jnp.int32(0)
    for a, b in caps[:-1]:
        tier += jnp.where((need[0] > a) | (need[1] > b), 1, 0)
    out[0] = tier


def run_tier(cnt, caps):
    return pl.pallas_call(functools.partial(tier_kernel, caps), out_shape=jax.ShapeDtypeStruct((1,), jnp.int32), in_specs=[SMEM], out_specs=SMEM, name="tier")(cnt)


def solution(mesh):
    tok_spec = P(('dp', 'ep'), None)
    swap_x = [(0, 2), (2, 0), (1, 3), (3, 1)]
    swap_c = [(0, 1), (1, 0), (2, 3), (3, 2)]

    def local_block(tokens, expert_ids, norm_gain, router_w, w_gate, w_up, w_down):
        num_tok, dim = tokens.shape
        quarter = num_tok // 4
        gain = norm_gain.astype(jnp.float32)
        me = lax.axis_index('ep').astype(jnp.int32)
        half = lax.axis_index('tp').astype(jnp.int32)
        pos = jnp.stack([me, half])

        own_h, logits = [], []
        for q in range(4):
            x = tokens[q * quarter:(q + 1) * quarter].astype(jnp.float32)
            inv = lax.rsqrt(jnp.mean(x * x, axis=-1, keepdims=True) + NORM_EPS)
            h = (x * inv * gain).astype(jnp.bfloat16)
            own_h.append(h)
            logits.append(jnp.dot(h, router_w, preferred_element_type=jnp.float32))
        logits = jnp.concatenate(logits, axis=0)
        exps = jnp.arange(8, dtype=jnp.int32)
        hit = expert_ids[:, :, None] == exps[None, None, :]
        gates = jax.nn.softmax(jnp.sum(jnp.where(hit, logits[:, None, :], 0.0), axis=-1), axis=-1)
        gate_of = jnp.sum(jnp.where(hit, gates[:, :, None], 0.0), axis=1)

        ids = lax.all_gather(expert_ids.T, 'ep')
        chosen = (ids[:, 0, None, :] == exps[None, :, None]) | (ids[:, 1, None, :] == exps[None, :, None])
        cnt = jnp.sum(chosen.reshape(4, 8, 8, PIECE).astype(jnp.int32), axis=-1).reshape(-1)
        tri = (jnp.arange(PIECE)[:, None] < jnp.arange(PIECE)[None, :]).astype(jnp.bfloat16)

        def ranked(picked):
            before = jnp.dot(picked.astype(jnp.bfloat16), tri, preferred_element_type=jnp.float32)
            return jnp.where(picked, before.astype(jnp.int32), -1)

        ids_rel = ids[me ^ jnp.arange(4, dtype=jnp.int32)]
        mine = 2 * me + jnp.arange(2, dtype=jnp.int32)
        picked = (ids_rel[:, 0, None, :] == mine[None, :, None]) | (ids_rel[:, 1, None, :] == mine[None, :, None])
        rank_in = ranked(picked.reshape(64, PIECE))
        own_picked = jnp.any(hit, axis=1).T
        rank_own = ranked(own_picked.reshape(64, PIECE)).reshape(8, num_tok).T

        def body(caps, tokens, own_h, pos, cnt, rank_in, rank_own, gate_of, w_gate, w_up, w_down):
            far_h = [lax.ppermute(h, 'ep', swap_x) for h in own_h]
            mate_h = [lax.ppermute(h, 'ep', swap_c) for h in own_h]
            far_mate_h = [lax.ppermute(h, 'ep', swap_c) for h in far_h]
            toks = [own_h, mate_h] + [[far_h[q], far_mate_h[q]] for q in range(4)]
            half = pos[1]
            out = jnp.zeros_like(tokens)
            rows, fulls, pieces = [], [], []

            def mix(q):
                at = q * quarter + half * PIECE

                def part(v):
                    return lax.dynamic_slice(v, (at, 0), (PIECE, v.shape[1]))

                piece = run_mix(q, pos, cnt, part(rank_own), part(gate_of), part(tokens), rows[0], rows[1], *rows[2 + q])
                pieces.append((piece, lax.ppermute(piece, 'tp', [(0, 1), (1, 0)])))

            for k in range(len(CHUNKS)):
                after = pos
                if k >= 2:
                    after = lax.optimization_barrier((pos, fulls[k - 2]))[0]
                if k == 5:
                    mix(0)
                    after = lax.optimization_barrier((after, pieces[0][0]))[0]
                send, keep = run_ffn(k, caps[0 if k < 2 else 1], after, cnt, rank_in, toks[k], w_gate, w_up, w_down)
                got = lax.ppermute(send, 'tp', [(0, 1), (1, 0)])
                full = (keep.astype(jnp.float32) + got.astype(jnp.float32)).astype(jnp.bfloat16)
                fulls.append(full)
                if k == 0:
                    rows.append(full)
                elif k == 1:
                    rows.append(lax.ppermute(full, 'ep', swap_c))
                else:
                    far = lax.ppermute(full, 'ep', swap_x)
                    rows.append((far, lax.ppermute(far, 'ep', swap_c)))
            for q in range(1, 4):
                mix(q)
            for q, (piece, other) in enumerate(pieces):
                out = lax.dynamic_update_slice(out, piece, (q * quarter + half * PIECE, 0))
                out = lax.dynamic_update_slice(out, other, (q * quarter + (1 - half) * PIECE, 0))
            return out

        args = (tokens, own_h, pos, cnt, rank_in, rank_own, gate_of, w_gate, w_up, w_down)
        if len(TIERS) == 1:
            return body(TIERS[0], *args)
        tier = run_tier(cnt, TIERS)
        return lax.switch(tier[0], [functools.partial(body, caps) for caps in TIERS], *args)

    return jax.shard_map(local_block, mesh=mesh, in_specs=(tok_spec, tok_spec, P(None), P(None, None), P('ep', None, 'tp'), P('ep', None, 'tp'), P('ep', 'tp', None)), out_specs=tok_spec, check_vma=False)
```

```python
import functools

import jax
import jax.numpy as jnp
from jax import lax
from jax.experimental import pallas as pl
from jax.experimental.pallas import tpu as pltpu
from jax.sharding import PartitionSpec as P

NORM_EPS = 1e-5
ALIGN = 16
PIECE = 512
SUB = 128
TILE = 512
FCH = 256
RP = 2304
ANY = pl.BlockSpec(memory_space=pl.ANY)
SMEM = pl.BlockSpec(memory_space=pltpu.SMEM)
VMEM = pl.BlockSpec(memory_space=pltpu.VMEM)
NQ = 2
PICK = 1152
TIERS = (1408, 1568, 2176)


def count_at(cnt, block, exp, quarter, half):
    return cnt[((block * 8 + exp) * 4 + quarter) * 2 + half]


def padded(c):
    return (c + (ALIGN - 1)) // ALIGN * ALIGN


def half_rows(cnt, block, exp, q0, half):
    return sum(padded(count_at(cnt, block, exp, q0 + a, half)) for a in range(NQ))


def ffn_kernel(rel, q0, groups, pos_ref, cnt_ref, rank_ref, *refs):
    n, ng = NQ, len(groups)
    toks, ws = refs[:n], [refs[n + 3 * i:n + 3 * i + 3] for i in range(ng)]
    send, keep, tokb, hbuf, acc, b1, b3, b2, tsem, wsem, osem = refs[-11:]
    me, half = pos_ref[0], pos_ref[1]
    block = me ^ rel
    nf = ws[0][0].shape[2] // FCH
    ntok = 2 * PIECE

    def w_copies(w, g):
        e, f, s = g // nf % 2, g % nf, g % 2
        cols = pl.ds(pl.multiple_of(f * FCH, FCH), FCH)
        return (pltpu.make_async_copy(w[0].at[e, :, cols], b1.at[s], wsem.at[s, 0]),
                pltpu.make_async_copy(w[1].at[e, :, cols], b3.at[s], wsem.at[s, 1]),
                pltpu.make_async_copy(w[2].at[e, cols, :], b2.at[s], wsem.at[s, 2]))

    def w_start(g):
        for i, w in enumerate(ws):
            @pl.when(g // (2 * nf) == i)
            def _():
                for c in w_copies(w, g):
                    c.start()

    def tok_copy(a):
        return pltpu.make_async_copy(toks[a], tokb.at[pl.ds(a * ntok, ntok)], tsem.at[a])

    for a in range(n):
        tok_copy(a).start()
    w_start(jnp.int32(0))
    for a in range(n):
        tok_copy(a).wait()

    def expert(e, bases):
        g_dev = groups[0] + e // 2
        exp = 2 * (me ^ g_dev) + e % 2

        def piece(p, row):
            t, a = jnp.where(p < n, 1 - half, half), p % n
            c = count_at(cnt_ref, block, exp, q0 + a, t)
            ranks = rank_ref[pl.ds(((rel // 2 * 4 + g_dev * 2 + e % 2) * 4 + q0 + a) * 2 + t, 1), :]
            tok = pl.ds(pl.multiple_of(a * ntok + t * PIECE, PIECE), PIECE)

            def sub(s, _):
                rows = lax.broadcasted_iota(jnp.int32, (SUB, PIECE), 0) + s * SUB
                sel = jnp.where(rows == ranks, 1.0, 0.0).astype(jnp.bfloat16)
                got = jnp.dot(sel, tokb[tok, :], preferred_element_type=jnp.float32)
                hbuf[pl.ds(pl.multiple_of(row + s * SUB, ALIGN), SUB), :] = got.astype(jnp.bfloat16)
                return 0

            lax.fori_loop(0, (c + SUB - 1) // SUB, sub, 0)
            return row + padded(c)

        first = lax.fori_loop(0, n, piece, jnp.int32(0))
        total = lax.fori_loop(n, 2 * n, piece, first)
        half_tile = TILE // 2
        nt = (total + half_tile - 1) // TILE
        rest = total > nt * TILE

        def tile(j, rows=TILE):
            return pl.ds(pl.multiple_of(j * TILE, TILE), rows)

        def over_tiles(do):
            pl.loop(0, nt)(lambda j: do(tile(j)))
            pl.when(rest)(lambda: do(tile(nt, half_tile)))

        def clear(at):
            acc[at, :] = jnp.zeros((at.size, acc.shape[1]), jnp.float32)

        over_tiles(clear)

        def width(f, _):
            g = e * nf + f
            s = g % 2

            w_start(g + 1)
            for c in w_copies(ws[0], g):
                c.wait()

            def rows(at):
                h = hbuf[at, :]
                a = jnp.dot(h, b1[s], preferred_element_type=jnp.float32)
                b = jnp.dot(h, b3[s], preferred_element_type=jnp.float32)
                u = (jax.nn.silu(a) * b).astype(jnp.bfloat16)
                acc[at, :] += jnp.dot(u, b2[s], preferred_element_type=jnp.float32)

            over_tiles(rows)
            return 0

        lax.fori_loop(0, nf, width, 0)

        def cast(at):
            hbuf[at, :] = acc[at, :].astype(jnp.bfloat16)

        over_tiles(cast)
        ends = []
        for dst, base, lo, hi in ((send, bases[0], 0, first), (keep, bases[1], first, total)):
            size = hi - lo
            whole = size // SUB

            def copy(at, rows):
                return pltpu.make_async_copy(hbuf.at[pl.ds(pl.multiple_of(lo + at, ALIGN), rows)],
                                             dst.at[pl.ds(pl.multiple_of(base + at, ALIGN), rows)], osem)

            def big(j, wait):
                c = copy(j * SUB, SUB)
                c.wait() if wait else c.start()

            def small(j, wait):
                c = copy(whole * SUB + j * ALIGN, ALIGN)
                c.wait() if wait else c.start()

            for wait in (False, True):
                pl.loop(0, whole)(lambda j: big(j, wait))
                pl.loop(0, (size - whole * SUB) // ALIGN)(lambda j: small(j, wait))
            ends.append(base + size)
        return tuple(ends)

    start = [jnp.int32(0), jnp.int32(0)]
    if groups[0]:
        for e in range(2):
            start[0] += half_rows(cnt_ref, block, 2 * me + e, q0, 1 - half)
            start[1] += half_rows(cnt_ref, block, 2 * me + e, q0, half)
    lax.fori_loop(0, 2 * ng, expert, tuple(start))


def run_ffn(rel, q0, groups, cap, pos, cnt, ranks, toks, weights, into=()):
    dim, width = weights[0][0].shape[1:]
    rows = 1024 * len(groups)
    flat = [w for ws in weights for w in ws]
    n_in = 3 + NQ + len(flat)
    kern = functools.partial(ffn_kernel, rel, q0, groups)
    if into:
        def kern(*refs):
            ffn_kernel(rel, q0, groups, *refs[:n_in], *refs[n_in + 2:])
    return pl.pallas_call(
        kern,
        out_shape=[jax.ShapeDtypeStruct((cap, dim), jnp.bfloat16)] * 2,
        in_specs=[SMEM, SMEM, VMEM] + [ANY] * (NQ + len(flat) + len(into)),
        out_specs=[ANY, ANY],
        input_output_aliases={n_in: 0, n_in + 1: 1} if into else {},
        scratch_shapes=[
            pltpu.VMEM((NQ * 2 * PIECE, dim), jnp.bfloat16),
            pltpu.VMEM((RP, dim), jnp.bfloat16),
            pltpu.VMEM((RP, dim), jnp.float32),
            pltpu.VMEM((2, dim, FCH), jnp.bfloat16),
            pltpu.VMEM((2, dim, FCH), jnp.bfloat16),
            pltpu.VMEM((2, FCH, dim), jnp.bfloat16),
            pltpu.SemaphoreType.DMA((NQ,)),
            pltpu.SemaphoreType.DMA((2, 3)),
            pltpu.SemaphoreType.DMA,
        ],
        compiler_params=pltpu.CompilerParams(vmem_limit_bytes=60 * 1024 * 1024),
        cost_estimate=pl.CostEstimate(flops=rows * 6 * dim * width, bytes_accessed=6 * dim * width * 2 * len(groups), transcendentals=0),
        name=f"ffn_r{rel}q{q0}g{groups[0]}",
    )(pos, cnt, ranks, *toks, *flat, *into)


def mix_kernel(quarter, pos_ref, cnt_ref, ranks, ids, gates, tokens, own, far, out, rb, xb, sem, xsem):
    me, half = pos_ref[0], pos_ref[1]
    dim = out.shape[1]
    q0 = quarter // NQ * NQ
    row0 = quarter * 2 * PIECE + half * PIECE
    x_copy = pltpu.make_async_copy(tokens.at[pl.ds(pl.multiple_of(row0, PIECE), PIECE)], xb, xsem)
    x_copy.start()

    moves, shifts = [], []
    to = jnp.int32(0)
    for r, buf in ((0, own), (2, far)):
        at = jnp.int32(0)
        for g in range(2):
            for e in range(2):
                exp = 2 * (me ^ (r + g)) + e
                skip = jnp.int32(0)
                for q in range(q0, quarter):
                    skip += padded(count_at(cnt_ref, me, exp, q, half))
                size = padded(count_at(cnt_ref, me, exp, quarter, half))
                moves.append((buf, at + skip, to, size))
                shifts.append((exp, to))
                at += half_rows(cnt_ref, me, exp, q0, half)
                to += size

    for wait in (False, True):
        for buf, src, dst, size in moves:
            whole = size // SUB

            def copy(off, rows):
                c = pltpu.make_async_copy(buf.at[pl.ds(pl.multiple_of(src + off, ALIGN), rows)],
                                          rb.at[pl.ds(pl.multiple_of(dst + off, ALIGN), rows)], sem)
                c.wait() if wait else c.start()

            pl.loop(0, whole)(lambda j: copy(j * SUB, SUB))
            pl.loop(0, (size - whole * SUB) // ALIGN)(lambda j: copy(whole * SUB + j * ALIGN, ALIGN))
    x_copy.wait()

    tail = pl.ds(2 * PIECE, PICK - 2 * PIECE)
    valid = lax.broadcasted_iota(jnp.int32, (PICK - 2 * PIECE, dim), 0) + 2 * PIECE < to
    rb[tail, :] = jnp.where(valid, rb[tail, :].astype(jnp.float32), 0.0).astype(jnp.bfloat16)

    lane = lax.broadcasted_iota(jnp.int32, ranks.shape, 1)
    places = ranks[...]
    for exp, shift in shifts:
        places += jnp.where(lane == exp, shift, 0)
    n_col = 512
    sels = []
    for k in range(2):
        place = jnp.sum(jnp.where(lane == ids[:, k:k + 1], places, 0), axis=1, keepdims=True)
        col = lax.broadcasted_iota(jnp.int32, (PIECE, PICK), 1)
        sels.append(jnp.where(col == place, 1.0, 0.0).astype(jnp.bfloat16))
    for c in range(0, dim, n_col):
        cols = slice(c, c + n_col)
        mixed = xb[:, cols].astype(jnp.float32)
        for k in range(2):
            mixed += gates[:, k:k + 1] * jnp.dot(sels[k], rb[:, cols], preferred_element_type=jnp.float32)
        out[:, cols] = mixed.astype(out.dtype)


def run_mix(quarter, pos, cnt, ranks, ids, gates, tokens, own, far):
    dim = tokens.shape[1]
    return pl.pallas_call(
        functools.partial(mix_kernel, quarter),
        out_shape=jax.ShapeDtypeStruct((PIECE, dim), tokens.dtype),
        in_specs=[SMEM, SMEM, VMEM, VMEM, VMEM, ANY, ANY, ANY],
        out_specs=VMEM,
        scratch_shapes=[pltpu.VMEM((PICK, dim), jnp.bfloat16), pltpu.VMEM((PIECE, dim), jnp.bfloat16), pltpu.SemaphoreType.DMA, pltpu.SemaphoreType.DMA],
        cost_estimate=pl.CostEstimate(flops=4 * PIECE * PICK * dim, bytes_accessed=4 * PICK * dim, transcendentals=0),
        name=f"mix{quarter}",
    )(pos, cnt, ranks, ids, gates, tokens, own, far)


def tier_kernel(caps, cnt_ref, out):
    def group(i, m):
        block, chip, half = i // 4, i // 2 % 2, i % 2
        for q0 in range(0, 4, NQ):
            m = jnp.maximum(m, sum(half_rows(cnt_ref, block, 4 * chip + e, q0, half) for e in range(4)))
        return m

    need = lax.fori_loop(0, 16, group, jnp.int32(0))
    out[0] = sum(jnp.where(need > cap, 1, 0) for cap in caps[:-1])


def run_tier(cnt, caps):
    return pl.pallas_call(functools.partial(tier_kernel, caps), out_shape=jax.ShapeDtypeStruct((1,), jnp.int32), in_specs=[SMEM], out_specs=SMEM, name="tier")(cnt)


def solution(mesh):
    tok_spec = P(('dp', 'ep'), None)
    swap_x = [(0, 2), (2, 0), (1, 3), (3, 1)]
    swap_c = [(0, 1), (1, 0), (2, 3), (3, 2)]

    def local_block(tokens, expert_ids, norm_gain, router_w, w_gate, w_up, w_down):
        num_tok, dim = tokens.shape
        quarter = num_tok // 4
        gain = norm_gain.astype(jnp.float32)
        me = lax.axis_index('ep').astype(jnp.int32)
        half = lax.axis_index('tp').astype(jnp.int32)
        pos = jnp.stack([me, half])

        own_h, logits = [], []
        for q in range(4):
            x = tokens[q * quarter:(q + 1) * quarter].astype(jnp.float32)
            inv = lax.rsqrt(jnp.mean(x * x, axis=-1, keepdims=True) + NORM_EPS)
            h = (x * inv * gain).astype(jnp.bfloat16)
            own_h.append(h)
            logits.append(jnp.dot(h, router_w, preferred_element_type=jnp.float32))
        logits = jnp.concatenate(logits, axis=0)
        exps = jnp.arange(8, dtype=jnp.int32)
        hit = expert_ids[:, :, None] == exps[None, None, :]
        gates = jax.nn.softmax(jnp.sum(jnp.where(hit, logits[:, None, :], 0.0), axis=-1), axis=-1)

        ids = lax.all_gather(expert_ids.T, 'ep')
        chosen = (ids[:, 0, None, :] == exps[None, :, None]) | (ids[:, 1, None, :] == exps[None, :, None])
        cnt = jnp.sum(chosen.reshape(4, 8, 8, PIECE).astype(jnp.int32), axis=-1).reshape(-1)
        tri = (jnp.arange(PIECE)[:, None] < jnp.arange(PIECE)[None, :]).astype(jnp.bfloat16)

        def ranked(picked):
            before = jnp.dot(picked.astype(jnp.bfloat16), tri, preferred_element_type=jnp.float32)
            return jnp.where(picked, before.astype(jnp.int32), -1)

        ids_rel = ids[me ^ jnp.array([0, 2], jnp.int32)]
        mine = jnp.stack([2 * me, 2 * me + 1, 2 * (me ^ 1), 2 * (me ^ 1) + 1])
        picked = (ids_rel[:, 0, None, :] == mine[None, :, None]) | (ids_rel[:, 1, None, :] == mine[None, :, None])
        rank_in = ranked(picked.reshape(64, PIECE))
        own_picked = jnp.any(hit, axis=1).T
        rank_own = ranked(own_picked.reshape(64, PIECE)).reshape(8, num_tok).T

        def body(cap, tokens, own_h, pos, cnt, rank_in, rank_own, ids_own, gates, w_gate, w_up, w_down):
            far_h = [lax.ppermute(h, 'ep', swap_x) for h in own_h]
            mine = (w_gate, w_up, w_down)
            theirs = tuple(lax.ppermute(w, 'ep', swap_c) for w in mine)
            half = pos[1]
            out = jnp.zeros_like(tokens)
            pieces = []

            def ffn(rel, q0, groups, after, into=()):
                first = lax.optimization_barrier((pos, *after))[0]
                src = (own_h, far_h)[rel // 2][q0:q0 + NQ]
                return run_ffn(rel, q0, groups, cap, first, cnt, rank_in, src, [(mine, theirs)[g] for g in groups], into)

            def reduce(parts):
                got = lax.ppermute(parts[0], 'tp', [(0, 1), (1, 0)])
                return (parts[1].astype(jnp.float32) + got.astype(jnp.float32)).astype(jnp.bfloat16)

            def mix(q, own, far):
                piece = run_mix(q, pos, cnt, rank_own[q], ids_own[q], gates[q], tokens, own, far)
                pieces.append((piece, lax.ppermute(piece, 'tp', [(0, 1), (1, 0)])))

            a0 = ffn(0, 0, (0,), ())
            a1 = ffn(0, 2, (0,), a0[:1])
            a0 = ffn(0, 0, (1,), a1[:1], a0)
            full_a0 = reduce(a0)
            a1 = ffn(0, 2, (1,), a0[:1], a1)
            full_a1 = reduce(a1)
            b0 = ffn(2, 0, (0, 1), a1[:1])
            full_b0 = reduce(b0)
            b1 = ffn(2, 2, (0, 1), (b0[0], full_a0))
            full_b1 = reduce(b1)
            back_b0 = lax.ppermute(full_b0, 'ep', swap_x)
            back_b1 = lax.ppermute(full_b1, 'ep', swap_x)
            for q in range(4):
                mix(q, (full_a0, full_a1)[q // NQ], (back_b0, back_b1)[q // NQ])
            for q, (piece, other) in enumerate(pieces):
                out = lax.dynamic_update_slice(out, piece, (q * quarter + half * PIECE, 0))
                out = lax.dynamic_update_slice(out, other, (q * quarter + (1 - half) * PIECE, 0))
            return out

        def own_half(v):
            return lax.dynamic_index_in_dim(v.reshape(4, 2, PIECE, -1), half, 1, keepdims=False)

        args = (tokens, own_h, pos, cnt, rank_in, own_half(rank_own), own_half(expert_ids), own_half(gates), w_gate, w_up, w_down)
        if len(TIERS) == 1:
            return body(TIERS[0], *args)
        tier = run_tier(cnt, TIERS)
        return lax.switch(tier[0], [functools.partial(body, caps) for caps in TIERS], *args)

    return jax.shard_map(local_block, mesh=mesh, in_specs=(tok_spec, tok_spec, P(None), P(None, None), P('ep', None, 'tp'), P('ep', None, 'tp'), P('ep', 'tp', None)), out_specs=tok_spec, check_vma=False)
```

```python
import functools

import jax
import jax.numpy as jnp
from jax import lax
from jax.experimental import pallas as pl
from jax.experimental.pallas import tpu as pltpu
from jax.sharding import PartitionSpec as P


NORM_EPS = 1e-5
ALIGN = 16
PIECE = 512
SUB = 128
TILE = 512
FCH = 256
RP = 2304
ANY = pl.BlockSpec(memory_space=pl.ANY)
SMEM = pl.BlockSpec(memory_space=pltpu.SMEM)
VMEM = pl.BlockSpec(memory_space=pltpu.VMEM)
PICK = 1152
TIERS = (688, 736, 784, 848, 1088)


def count_at(cnt, block, exp, quarter, half):
    return cnt[((block * 8 + exp) * 4 + quarter) * 2 + half]


def padded(c):
    return (c + (ALIGN - 1)) // ALIGN * ALIGN


def ffn_kernel(rel, q0, n, groups, pos_ref, cnt_ref, rank_ref, *refs):
    ng = len(groups)
    toks, ws = refs[:n], [refs[n + 3 * i:n + 3 * i + 3] for i in range(ng)]
    outs, (tokb, hbuf, acc, b1, b3, b2, tsem, wsem, osem) = refs[-9 - 2 * n:-9], refs[-9:]
    me, half = pos_ref[0], pos_ref[1]
    block = me ^ rel
    nf = ws[0][0].shape[2] // FCH
    ntok = 2 * PIECE

    def w_copies(w, g):
        e, f, s = g // nf % 2, g % nf, g % 2
        cols = pl.ds(pl.multiple_of(f * FCH, FCH), FCH)
        return (pltpu.make_async_copy(w[0].at[e, :, cols], b1.at[s], wsem.at[s, 0]),
                pltpu.make_async_copy(w[1].at[e, :, cols], b3.at[s], wsem.at[s, 1]),
                pltpu.make_async_copy(w[2].at[e, cols, :], b2.at[s], wsem.at[s, 2]))

    def w_start(g):
        for i, w in enumerate(ws):
            @pl.when(g // (2 * nf) == i)
            def _():
                for c in w_copies(w, g):
                    c.start()

    def tok_copy(a):
        return pltpu.make_async_copy(toks[a], tokb.at[pl.ds(a * ntok, ntok)], tsem.at[a])

    for a in range(n):
        tok_copy(a).start()
    w_start(jnp.int32(0))
    for a in range(n):
        tok_copy(a).wait()

    def expert(e, bases):
        g_dev = groups[0] + e // 2
        exp = 2 * (me ^ g_dev) + e % 2

        def piece(p, row):
            t, a = jnp.where(p < n, 1 - half, half), p % n
            c = count_at(cnt_ref, block, exp, q0 + a, t)
            ranks = rank_ref[pl.ds(((rel // 2 * 4 + g_dev * 2 + e % 2) * 4 + q0 + a) * 2 + t, 1), :]
            tok = pl.ds(pl.multiple_of(a * ntok + t * PIECE, PIECE), PIECE)

            def sub(s, _):
                rows = lax.broadcasted_iota(jnp.int32, (SUB, PIECE), 0) + s * SUB
                sel = jnp.where(rows == ranks, 1.0, 0.0).astype(jnp.bfloat16)
                got = jnp.dot(sel, tokb[tok, :], preferred_element_type=jnp.float32)
                hbuf[pl.ds(pl.multiple_of(row + s * SUB, ALIGN), SUB), :] = got.astype(jnp.bfloat16)
                return 0

            lax.fori_loop(0, (c + SUB - 1) // SUB, sub, 0)
            return row + padded(c)

        total = lax.fori_loop(0, 2 * n, piece, jnp.int32(0))
        half_tile = TILE // 2
        nt = (total + half_tile - 1) // TILE
        rest = total > nt * TILE

        def tile(j, rows=TILE):
            return pl.ds(pl.multiple_of(j * TILE, TILE), rows)

        def over_tiles(do):
            pl.loop(0, nt)(lambda j: do(tile(j)))
            pl.when(rest)(lambda: do(tile(nt, half_tile)))

        def clear(at):
            acc[at, :] = jnp.zeros((at.size, acc.shape[1]), jnp.float32)

        over_tiles(clear)

        def width(f, _):
            g = e * nf + f
            s = g % 2

            w_start(g + 1)
            for c in w_copies(ws[0], g):
                c.wait()

            def rows(at):
                h = hbuf[at, :]
                a = jnp.dot(h, b1[s], preferred_element_type=jnp.float32)
                b = jnp.dot(h, b3[s], preferred_element_type=jnp.float32)
                u = (jax.nn.silu(a) * b).astype(jnp.bfloat16)
                acc[at, :] += jnp.dot(u, b2[s], preferred_element_type=jnp.float32)

            over_tiles(rows)
            return 0

        lax.fori_loop(0, nf, width, 0)

        def cast(at):
            hbuf[at, :] = acc[at, :].astype(jnp.bfloat16)

        over_tiles(cast)
        ends, lo = [], jnp.int32(0)
        places = []
        for p in range(2 * n):
            size = padded(count_at(cnt_ref, block, exp, q0 + p % n, 1 - half if p < n else half))
            places.append((outs[p], bases[p], lo, size))
            ends.append(bases[p] + size)
            lo += size
        for wait in (False, True):
            for dst, base, lo, size in places:
                whole = size // SUB

                def copy(at, rows):
                    c = pltpu.make_async_copy(hbuf.at[pl.ds(pl.multiple_of(lo + at, ALIGN), rows)],
                                              dst.at[pl.ds(pl.multiple_of(base + at, ALIGN), rows)], osem)
                    c.wait() if wait else c.start()

                pl.loop(0, whole)(lambda j: copy(j * SUB, SUB))
                pl.loop(0, (size - whole * SUB) // ALIGN)(lambda j: copy(whole * SUB + j * ALIGN, ALIGN))
        return tuple(ends)

    start = []
    for p in range(2 * n):
        at = jnp.int32(0)
        if groups[0]:
            for e in range(2):
                at += padded(count_at(cnt_ref, block, 2 * me + e, q0 + p % n, 1 - half if p < n else half))
        start.append(at)
    lax.fori_loop(0, 2 * ng, expert, tuple(start))


def run_ffn(rel, q0, n, groups, cap, pos, cnt, ranks, toks, weights, into=()):
    dim, width = weights[0][0].shape[1:]
    rows = 512 * n * len(groups)
    flat = [w for ws in weights for w in ws]
    n_in = 3 + n + len(flat)
    kern = functools.partial(ffn_kernel, rel, q0, n, groups)
    if into:
        def kern(*refs):
            ffn_kernel(rel, q0, n, groups, *refs[:n_in], *refs[n_in + 2 * n:])
    return pl.pallas_call(
        kern,
        out_shape=[jax.ShapeDtypeStruct((cap, dim), jnp.bfloat16)] * (2 * n),
        in_specs=[SMEM, SMEM, VMEM] + [ANY] * (n + len(flat) + len(into)),
        out_specs=[ANY] * (2 * n),
        input_output_aliases={n_in + i: i for i in range(len(into))},
        scratch_shapes=[
            pltpu.VMEM((n * 2 * PIECE, dim), jnp.bfloat16),
            pltpu.VMEM((RP, dim), jnp.bfloat16),
            pltpu.VMEM((RP, dim), jnp.float32),
            pltpu.VMEM((2, dim, FCH), jnp.bfloat16),
            pltpu.VMEM((2, dim, FCH), jnp.bfloat16),
            pltpu.VMEM((2, FCH, dim), jnp.bfloat16),
            pltpu.SemaphoreType.DMA((n,)),
            pltpu.SemaphoreType.DMA((2, 3)),
            pltpu.SemaphoreType.DMA,
        ],
        compiler_params=pltpu.CompilerParams(vmem_limit_bytes=62 * 1024 * 1024),
        cost_estimate=pl.CostEstimate(flops=rows * 6 * dim * width, bytes_accessed=6 * dim * width * 2 * len(groups), transcendentals=0),
    )(pos, cnt, ranks, *toks, *flat, *into)


def mix_kernel(quarter, pos_ref, cnt_ref, ranks, ids, gates, tokens, own, far, out, rb, xb, sem, xsem):
    me, half = pos_ref[0], pos_ref[1]
    dim = out.shape[1]
    row0 = quarter * 2 * PIECE + half * PIECE
    x_copy = pltpu.make_async_copy(tokens.at[pl.ds(pl.multiple_of(row0, PIECE), PIECE)], xb, xsem)
    x_copy.start()

    moves, shifts = [], []
    to = jnp.int32(0)
    for r, buf in ((0, own), (2, far)):
        at = jnp.int32(0)
        for g in range(2):
            for e in range(2):
                exp = 2 * (me ^ (r + g)) + e
                size = padded(count_at(cnt_ref, me, exp, quarter, half))
                moves.append((buf, at, to, size))
                shifts.append((exp, to))
                at += size
                to += size

    for wait in (False, True):
        for buf, src, dst, size in moves:
            whole = size // SUB

            def copy(off, rows):
                c = pltpu.make_async_copy(buf.at[pl.ds(pl.multiple_of(src + off, ALIGN), rows)],
                                          rb.at[pl.ds(pl.multiple_of(dst + off, ALIGN), rows)], sem)
                c.wait() if wait else c.start()

            pl.loop(0, whole)(lambda j: copy(j * SUB, SUB))
            pl.loop(0, (size - whole * SUB) // ALIGN)(lambda j: copy(whole * SUB + j * ALIGN, ALIGN))
    x_copy.wait()

    tail = pl.ds(2 * PIECE, PICK - 2 * PIECE)
    valid = lax.broadcasted_iota(jnp.int32, (PICK - 2 * PIECE, dim), 0) + 2 * PIECE < to
    rb[tail, :] = jnp.where(valid, rb[tail, :].astype(jnp.float32), 0.0).astype(jnp.bfloat16)

    lane = lax.broadcasted_iota(jnp.int32, ranks.shape, 1)
    places = ranks[...]
    for exp, shift in shifts:
        places += jnp.where(lane == exp, shift, 0)
    n_col = 512
    sels = []
    for k in range(2):
        place = jnp.sum(jnp.where(lane == ids[:, k:k + 1], places, 0), axis=1, keepdims=True)
        col = lax.broadcasted_iota(jnp.int32, (PIECE, PICK), 1)
        sels.append(jnp.where(col == place, 1.0, 0.0).astype(jnp.bfloat16))
    for c in range(0, dim, n_col):
        cols = slice(c, c + n_col)
        mixed = xb[:, cols].astype(jnp.float32)
        for k in range(2):
            mixed += gates[:, k:k + 1] * jnp.dot(sels[k], rb[:, cols], preferred_element_type=jnp.float32)
        out[:, cols] = mixed.astype(out.dtype)


def run_mix(quarter, pos, cnt, ranks, ids, gates, tokens, own, far):
    dim = tokens.shape[1]
    return pl.pallas_call(
        functools.partial(mix_kernel, quarter),
        out_shape=jax.ShapeDtypeStruct((PIECE, dim), tokens.dtype),
        in_specs=[SMEM, SMEM, VMEM, VMEM, VMEM, ANY, ANY, ANY],
        out_specs=VMEM,
        scratch_shapes=[pltpu.VMEM((PICK, dim), jnp.bfloat16), pltpu.VMEM((PIECE, dim), jnp.bfloat16), pltpu.SemaphoreType.DMA, pltpu.SemaphoreType.DMA],
        cost_estimate=pl.CostEstimate(flops=4 * PIECE * PICK * dim, bytes_accessed=4 * PICK * dim, transcendentals=0),
    )(pos, cnt, ranks, ids, gates, tokens, own, far)


def tier_kernel(caps, cnt_ref, out):
    def group(i, m):
        block, chip, quarter, half = i // 16, i // 8 % 2, i // 2 % 4, i % 2
        return jnp.maximum(m, sum(padded(count_at(cnt_ref, block, 4 * chip + e, quarter, half)) for e in range(4)))

    need = lax.fori_loop(0, 64, group, jnp.int32(0))
    out[0] = sum(jnp.where(need > cap, 1, 0) for cap in caps[:-1])


def run_tier(cnt, caps):
    return pl.pallas_call(functools.partial(tier_kernel, caps), out_shape=jax.ShapeDtypeStruct((1,), jnp.int32), in_specs=[SMEM], out_specs=SMEM, name="tier")(cnt)


def solution(mesh):
    tok_spec = P(('dp', 'ep'), None)
    swap_x = [(0, 2), (2, 0), (1, 3), (3, 1)]
    swap_c = [(0, 1), (1, 0), (2, 3), (3, 2)]

    def local_block(tokens, expert_ids, norm_gain, router_w, w_gate, w_up, w_down):
        num_tok, _ = tokens.shape
        quarter = num_tok // 4
        gain = norm_gain.astype(jnp.float32)
        me = lax.axis_index('ep').astype(jnp.int32)
        half = lax.axis_index('tp').astype(jnp.int32)
        pos = jnp.stack([me, half])

        own_h, logits = [], []
        for q in range(4):
            x = tokens[q * quarter:(q + 1) * quarter].astype(jnp.float32)
            inv = lax.rsqrt(jnp.mean(x * x, axis=-1, keepdims=True) + NORM_EPS)
            h = (x * inv * gain).astype(jnp.bfloat16)
            own_h.append(h)
            logits.append(jnp.dot(h, router_w, preferred_element_type=jnp.float32))
        logits = jnp.concatenate(logits, axis=0)
        exps = jnp.arange(8, dtype=jnp.int32)
        hit = expert_ids[:, :, None] == exps[None, None, :]
        gates = jax.nn.softmax(jnp.sum(jnp.where(hit, logits[:, None, :], 0.0), axis=-1), axis=-1)

        ids = lax.all_gather(expert_ids.T, 'ep')
        chosen = (ids[:, 0, None, :] == exps[None, :, None]) | (ids[:, 1, None, :] == exps[None, :, None])
        cnt = jnp.sum(chosen.reshape(4, 8, 8, PIECE).astype(jnp.int32), axis=-1).reshape(-1)
        tri = (jnp.arange(PIECE)[:, None] < jnp.arange(PIECE)[None, :]).astype(jnp.bfloat16)

        def ranked(picked):
            before = jnp.dot(picked.astype(jnp.bfloat16), tri, preferred_element_type=jnp.float32)
            return jnp.where(picked, before.astype(jnp.int32), -1)

        ids_rel = ids[me ^ jnp.array([0, 2], jnp.int32)]
        mine = jnp.stack([2 * me, 2 * me + 1, 2 * (me ^ 1), 2 * (me ^ 1) + 1])
        picked = (ids_rel[:, 0, None, :] == mine[None, :, None]) | (ids_rel[:, 1, None, :] == mine[None, :, None])
        rank_in = ranked(picked.reshape(64, PIECE))
        own_picked = jnp.any(hit, axis=1).T
        rank_own = ranked(own_picked.reshape(64, PIECE)).reshape(8, num_tok).T

        def body(cap, tokens, own_h, pos, cnt, rank_in, rank_own, ids_own, gates, w_gate, w_up, w_down):
            far_h = [lax.ppermute(h, 'ep', swap_x) for h in own_h]
            mine = (w_gate, w_up, w_down)
            theirs = tuple(lax.ppermute(w, 'ep', swap_c) for w in mine)
            half = pos[1]
            out = jnp.zeros_like(tokens)
            pieces = []

            def ffn(rel, q0, n, groups, after, into=()):
                first = lax.optimization_barrier((pos, *after))[0]
                src = (own_h, far_h)[rel // 2][q0:q0 + n]
                return run_ffn(rel, q0, n, groups, cap, first, cnt, rank_in, src, [(mine, theirs)[g] for g in groups], into)

            def swap_tp(send):
                return lax.ppermute(send, 'tp', [(0, 1), (1, 0)])

            def reduce(send, keep):
                got = swap_tp(send)
                return (keep.astype(jnp.float32) + got.astype(jnp.float32)).astype(jnp.bfloat16)

            def mix(q, own, far):
                piece = run_mix(q, pos, cnt, rank_own[q], ids_own[q], gates[q], tokens, own, far)
                pieces.append((piece, lax.ppermute(piece, 'tp', [(0, 1), (1, 0)])))

            a = ffn(0, 0, 4, (0,), ())
            send, keep = a[:4], a[4:]
            a0 = ffn(0, 0, 2, (1,), a[:1], (*send[:2], *keep[:2]))
            own = [reduce(a0[i], a0[2 + i]) for i in range(2)]
            a1 = ffn(0, 2, 2, (1,), a0[:1], (*send[2:], *keep[2:]))
            own += [reduce(a1[i], a1[2 + i]) for i in range(2)]
            b0 = ffn(2, 0, 2, (0, 1), a1[:1])
            far = [reduce(b0[i], b0[2 + i]) for i in range(2)]
            b1 = ffn(2, 2, 2, (0, 1), b0[:1])
            late = [swap_tp(b1[i]) for i in range(2)]
            back = [lax.ppermute(rows, 'ep', swap_x) for rows in far]
            for i in range(2):
                mix(i, own[i], back[i])
                keep, got, _ = lax.optimization_barrier((b1[2 + i], late[i], pieces[i][0]))
                back.append(lax.ppermute((keep.astype(jnp.float32) + got.astype(jnp.float32)).astype(jnp.bfloat16), 'ep', swap_x))
            for q in range(2, 4):
                mix(q, own[q], back[q])
            for q, (piece, other) in enumerate(pieces):
                out = lax.dynamic_update_slice(out, piece, (q * quarter + half * PIECE, 0))
                out = lax.dynamic_update_slice(out, other, (q * quarter + (1 - half) * PIECE, 0))
            return out

        def own_half(v):
            return lax.dynamic_index_in_dim(v.reshape(4, 2, PIECE, -1), half, 1, keepdims=False)

        args = (tokens, own_h, pos, cnt, rank_in, own_half(rank_own), own_half(expert_ids), own_half(gates), w_gate, w_up, w_down)
        tier = run_tier(cnt, TIERS)

        def branch(i, *a):
            return body(TIERS[i], *a)

        return lax.switch(tier[0], [functools.partial(branch, i) for i in range(len(TIERS))], *args)

    return jax.shard_map(local_block, mesh=mesh, in_specs=(tok_spec, tok_spec, P(None), P(None, None), P('ep', None, 'tp'), P('ep', None, 'tp'), P('ep', 'tp', None)), out_specs=tok_spec, check_vma=False)
```

```python
import functools

import jax
import jax.numpy as jnp
from jax import lax
from jax.experimental import pallas as pl
from jax.experimental.pallas import tpu as pltpu
from jax.sharding import PartitionSpec as P


NORM_EPS = 1e-5
ALIGN = 16
PIECE = 512
SUB = 128
TILE = 512
FCH = 256
RP = 2304
ANY = pl.BlockSpec(memory_space=pl.ANY)
SMEM = pl.BlockSpec(memory_space=pltpu.SMEM)
VMEM = pl.BlockSpec(memory_space=pltpu.VMEM)
PICK = 1152
TIERS = (688, 736, 784, 848, 1088)


def count_at(cnt, block, exp, quarter, half):
    return cnt[((block * 8 + exp) * 4 + quarter) * 2 + half]


def padded(c):
    return (c + (ALIGN - 1)) // ALIGN * ALIGN


def ffn_kernel(rel, q0, n, groups, pos_ref, cnt_ref, rank_ref, *refs):
    ng = len(groups)
    toks, ws = refs[:n], [refs[n + 3 * i:n + 3 * i + 3] for i in range(ng)]
    outs, (tokb, hbuf, stage, acc, b1, b3, b2, tsem, wsem, osem) = refs[-10 - 2 * n:-10], refs[-10:]
    apart = n <= 2
    stage = stage if apart else hbuf
    me, half = pos_ref[0], pos_ref[1]
    block = me ^ rel
    nf = ws[0][0].shape[2] // FCH
    ntok = 2 * PIECE

    def w_copies(w, g):
        e, f, s = g // nf % 2, g % nf, g % 2
        cols = pl.ds(pl.multiple_of(f * FCH, FCH), FCH)
        return (pltpu.make_async_copy(w[0].at[e, :, cols], b1.at[s], wsem.at[s, 0]),
                pltpu.make_async_copy(w[1].at[e, :, cols], b3.at[s], wsem.at[s, 1]),
                pltpu.make_async_copy(w[2].at[e, cols, :], b2.at[s], wsem.at[s, 2]))

    def w_start(g):
        for i, w in enumerate(ws):
            @pl.when(g // (2 * nf) == i)
            def _():
                for c in w_copies(w, g):
                    c.start()

    def tok_copy(a):
        return pltpu.make_async_copy(toks[a], tokb.at[pl.ds(a * ntok, ntok)], tsem.at[a])

    for a in range(n):
        tok_copy(a).start()
    w_start(jnp.int32(0))
    for a in range(n):
        tok_copy(a).wait()

    def expert(e, bases):
        g_dev = groups[0] + e // 2
        exp = 2 * (me ^ g_dev) + e % 2

        def piece(p, row):
            t, a = jnp.where(p < n, 1 - half, half), p % n
            c = count_at(cnt_ref, block, exp, q0 + a, t)
            ranks = rank_ref[pl.ds(((rel // 2 * 4 + g_dev * 2 + e % 2) * 4 + q0 + a) * 2 + t, 1), :]
            tok = pl.ds(pl.multiple_of(a * ntok + t * PIECE, PIECE), PIECE)

            def sub(s, _):
                rows = lax.broadcasted_iota(jnp.int32, (SUB, PIECE), 0) + s * SUB
                sel = jnp.where(rows == ranks, 1.0, 0.0).astype(jnp.bfloat16)
                got = jnp.dot(sel, tokb[tok, :], preferred_element_type=jnp.float32)
                hbuf[pl.ds(pl.multiple_of(row + s * SUB, ALIGN), SUB), :] = got.astype(jnp.bfloat16)
                return 0

            lax.fori_loop(0, (c + SUB - 1) // SUB, sub, 0)
            return row + padded(c)

        total = lax.fori_loop(0, 2 * n, piece, jnp.int32(0))
        half_tile = TILE // 2
        nt = (total + half_tile - 1) // TILE
        rest = total - nt * TILE

        def tile(j, rows=TILE):
            return pl.ds(pl.multiple_of(j * TILE, TILE), rows)

        def over_tiles(do):
            pl.loop(0, nt)(lambda j: do(tile(j)))
            pl.when(rest > half_tile // 2)(lambda: do(tile(nt, half_tile)))
            pl.when((rest > 0) & (rest <= half_tile // 2))(lambda: do(tile(nt, half_tile // 2)))

        def width(f, _):
            g = e * nf + f
            s = g % 2

            w_start(g + 1)
            for c in w_copies(ws[0], g):
                c.wait()

            def rows(at):
                h = hbuf[at, :]
                a = jnp.dot(h, b1[s], preferred_element_type=jnp.float32)
                b = jnp.dot(h, b3[s], preferred_element_type=jnp.float32)
                u = (jax.nn.silu(a) * b).astype(jnp.bfloat16)
                before = jnp.where(f > 0, acc[at, :], 0.0)
                acc[at, :] = before + jnp.dot(u, b2[s], preferred_element_type=jnp.float32)

            over_tiles(rows)
            return 0

        lax.fori_loop(0, nf, width, 0)

        @pl.when((e > 0) & apart)
        def _():
            move(e - 1, bases, True)

        def cast(at):
            stage[at, :] = acc[at, :].astype(jnp.bfloat16)

        over_tiles(cast)
        ends = move(e, bases, False)
        if not apart:
            move(e, ends, True)
        return ends

    def move(e, bases, wait):
        exp = 2 * (me ^ (groups[0] + e // 2)) + e % 2
        ends, lo = [], jnp.int32(0)
        for p in range(2 * n):
            size = padded(count_at(cnt_ref, block, exp, q0 + p % n, 1 - half if p < n else half))
            base = bases[p] - size if wait else bases[p]
            whole = size // SUB

            def copy(at, rows):
                c = pltpu.make_async_copy(stage.at[pl.ds(pl.multiple_of(lo + at, ALIGN), rows)],
                                          outs[p].at[pl.ds(pl.multiple_of(base + at, ALIGN), rows)], osem)
                c.wait() if wait else c.start()

            pl.loop(0, whole)(lambda j: copy(j * SUB, SUB))
            pl.loop(0, (size - whole * SUB) // ALIGN)(lambda j: copy(whole * SUB + j * ALIGN, ALIGN))
            ends.append(base + size)
            lo += size
        return tuple(ends)

    start = []
    for p in range(2 * n):
        at = jnp.int32(0)
        if groups[0]:
            for e in range(2):
                at += padded(count_at(cnt_ref, block, 2 * me + e, q0 + p % n, 1 - half if p < n else half))
        start.append(at)
    ends = lax.fori_loop(0, 2 * ng, expert, tuple(start))
    if apart:
        move(jnp.int32(2 * ng - 1), ends, True)


def run_ffn(rel, q0, n, groups, cap, pos, cnt, ranks, toks, weights, into=()):
    dim, width = weights[0][0].shape[1:]
    rows = 512 * n * len(groups)
    flat = [w for ws in weights for w in ws]
    n_in = 3 + n + len(flat)
    kern = functools.partial(ffn_kernel, rel, q0, n, groups)
    if into:
        def kern(*refs):
            ffn_kernel(rel, q0, n, groups, *refs[:n_in], *refs[n_in + 2 * n:])
    return pl.pallas_call(
        kern,
        out_shape=[jax.ShapeDtypeStruct((cap, dim), jnp.bfloat16)] * (2 * n),
        in_specs=[SMEM, SMEM, VMEM] + [ANY] * (n + len(flat) + len(into)),
        out_specs=[ANY] * (2 * n),
        input_output_aliases={n_in + i: i for i in range(len(into))},
        scratch_shapes=[
            pltpu.VMEM((n * 2 * PIECE, dim), jnp.bfloat16),
            pltpu.VMEM((RP, dim), jnp.bfloat16),
            pltpu.VMEM((RP if n <= 2 else ALIGN, dim), jnp.bfloat16),
            pltpu.VMEM((RP, dim), jnp.float32),
            pltpu.VMEM((2, dim, FCH), jnp.bfloat16),
            pltpu.VMEM((2, dim, FCH), jnp.bfloat16),
            pltpu.VMEM((2, FCH, dim), jnp.bfloat16),
            pltpu.SemaphoreType.DMA((n,)),
            pltpu.SemaphoreType.DMA((2, 3)),
            pltpu.SemaphoreType.DMA,
        ],
        compiler_params=pltpu.CompilerParams(vmem_limit_bytes=62 * 1024 * 1024),
        cost_estimate=pl.CostEstimate(flops=rows * 6 * dim * width, bytes_accessed=6 * dim * width * 2 * len(groups), transcendentals=0),
    )(pos, cnt, ranks, *toks, *flat, *into)


def mix_kernel(quarter, pos_ref, cnt_ref, ranks, ids, gates, tokens, own, far, out, rb, xb, sem, xsem):
    me, half = pos_ref[0], pos_ref[1]
    dim = out.shape[1]
    row0 = quarter * 2 * PIECE + half * PIECE
    x_copy = pltpu.make_async_copy(tokens.at[pl.ds(pl.multiple_of(row0, PIECE), PIECE)], xb, xsem)
    x_copy.start()

    moves, shifts = [], []
    to = jnp.int32(0)
    for r, buf in ((0, own), (2, far)):
        at = jnp.int32(0)
        for g in range(2):
            for e in range(2):
                exp = 2 * (me ^ (r + g)) + e
                size = padded(count_at(cnt_ref, me, exp, quarter, half))
                moves.append((buf, at, to, size))
                shifts.append((exp, to))
                at += size
                to += size

    for wait in (False, True):
        for buf, src, dst, size in moves:
            whole = size // SUB

            def copy(off, rows):
                c = pltpu.make_async_copy(buf.at[pl.ds(pl.multiple_of(src + off, ALIGN), rows)],
                                          rb.at[pl.ds(pl.multiple_of(dst + off, ALIGN), rows)], sem)
                c.wait() if wait else c.start()

            pl.loop(0, whole)(lambda j: copy(j * SUB, SUB))
            pl.loop(0, (size - whole * SUB) // ALIGN)(lambda j: copy(whole * SUB + j * ALIGN, ALIGN))
    x_copy.wait()

    tail = pl.ds(2 * PIECE, PICK - 2 * PIECE)
    valid = lax.broadcasted_iota(jnp.int32, (PICK - 2 * PIECE, dim), 0) + 2 * PIECE < to
    rb[tail, :] = jnp.where(valid, rb[tail, :].astype(jnp.float32), 0.0).astype(jnp.bfloat16)

    lane = lax.broadcasted_iota(jnp.int32, ranks.shape, 1)
    places = ranks[...]
    for exp, shift in shifts:
        places += jnp.where(lane == exp, shift, 0)
    n_col = 512
    sels = []
    for k in range(2):
        place = jnp.sum(jnp.where(lane == ids[:, k:k + 1], places, 0), axis=1, keepdims=True)
        col = lax.broadcasted_iota(jnp.int32, (PIECE, PICK), 1)
        sels.append(jnp.where(col == place, 1.0, 0.0).astype(jnp.bfloat16))
    for c in range(0, dim, n_col):
        cols = slice(c, c + n_col)
        mixed = xb[:, cols].astype(jnp.float32)
        for k in range(2):
            mixed += gates[:, k:k + 1] * jnp.dot(sels[k], rb[:, cols], preferred_element_type=jnp.float32)
        out[:, cols] = mixed.astype(out.dtype)


def run_mix(quarter, pos, cnt, ranks, ids, gates, tokens, own, far):
    dim = tokens.shape[1]
    return pl.pallas_call(
        functools.partial(mix_kernel, quarter),
        out_shape=jax.ShapeDtypeStruct((PIECE, dim), tokens.dtype),
        in_specs=[SMEM, SMEM, VMEM, VMEM, VMEM, ANY, ANY, ANY],
        out_specs=VMEM,
        scratch_shapes=[pltpu.VMEM((PICK, dim), jnp.bfloat16), pltpu.VMEM((PIECE, dim), jnp.bfloat16), pltpu.SemaphoreType.DMA, pltpu.SemaphoreType.DMA],
        cost_estimate=pl.CostEstimate(flops=4 * PIECE * PICK * dim, bytes_accessed=4 * PICK * dim, transcendentals=0),
    )(pos, cnt, ranks, ids, gates, tokens, own, far)


def tier_kernel(caps, cnt_ref, out):
    def group(i, m):
        block, chip, quarter, half = i // 16, i // 8 % 2, i // 2 % 4, i % 2
        return jnp.maximum(m, sum(padded(count_at(cnt_ref, block, 4 * chip + e, quarter, half)) for e in range(4)))

    need = lax.fori_loop(0, 64, group, jnp.int32(0))
    out[0] = sum(jnp.where(need > cap, 1, 0) for cap in caps[:-1])


def run_tier(cnt, caps):
    return pl.pallas_call(functools.partial(tier_kernel, caps), out_shape=jax.ShapeDtypeStruct((1,), jnp.int32), in_specs=[SMEM], out_specs=SMEM, name="tier")(cnt)


def solution(mesh):
    tok_spec = P(('dp', 'ep'), None)
    swap_x = [(0, 2), (2, 0), (1, 3), (3, 1)]
    swap_c = [(0, 1), (1, 0), (2, 3), (3, 2)]

    def local_block(tokens, expert_ids, norm_gain, router_w, w_gate, w_up, w_down):
        num_tok, _ = tokens.shape
        quarter = num_tok // 4
        gain = norm_gain.astype(jnp.float32)
        me = lax.axis_index('ep').astype(jnp.int32)
        half = lax.axis_index('tp').astype(jnp.int32)
        pos = jnp.stack([me, half])

        own_h, logits = [], []
        for q in range(4):
            x = tokens[q * quarter:(q + 1) * quarter].astype(jnp.float32)
            inv = lax.rsqrt(jnp.mean(x * x, axis=-1, keepdims=True) + NORM_EPS)
            h = (x * inv * gain).astype(jnp.bfloat16)
            own_h.append(h)
            logits.append(jnp.dot(h, router_w, preferred_element_type=jnp.float32))
        logits = jnp.concatenate(logits, axis=0)
        exps = jnp.arange(8, dtype=jnp.int32)
        hit = expert_ids[:, :, None] == exps[None, None, :]
        gates = jax.nn.softmax(jnp.sum(jnp.where(hit, logits[:, None, :], 0.0), axis=-1), axis=-1)

        ids = lax.all_gather(expert_ids.T, 'ep')
        chosen = (ids[:, 0, None, :] == exps[None, :, None]) | (ids[:, 1, None, :] == exps[None, :, None])
        cnt = jnp.sum(chosen.reshape(4, 8, 8, PIECE).astype(jnp.int32), axis=-1).reshape(-1)
        tri = (jnp.arange(PIECE)[:, None] < jnp.arange(PIECE)[None, :]).astype(jnp.bfloat16)

        def ranked(picked):
            before = jnp.dot(picked.astype(jnp.bfloat16), tri, preferred_element_type=jnp.float32)
            return jnp.where(picked, before.astype(jnp.int32), -1)

        ids_rel = ids[me ^ jnp.array([0, 2], jnp.int32)]
        mine = jnp.stack([2 * me, 2 * me + 1, 2 * (me ^ 1), 2 * (me ^ 1) + 1])
        picked = (ids_rel[:, 0, None, :] == mine[None, :, None]) | (ids_rel[:, 1, None, :] == mine[None, :, None])
        rank_in = ranked(picked.reshape(64, PIECE))
        own_picked = jnp.any(hit, axis=1).T
        rank_own = ranked(own_picked.reshape(64, PIECE)).reshape(8, num_tok).T

        def body(cap, tokens, own_h, pos, cnt, rank_in, rank_own, ids_own, gates, w_gate, w_up, w_down):
            far_h = [lax.ppermute(h, 'ep', swap_x) for h in own_h]
            mine = (w_gate, w_up, w_down)
            theirs = tuple(lax.ppermute(w, 'ep', swap_c) for w in mine)
            half = pos[1]
            out = jnp.zeros_like(tokens)
            pieces = []

            def ffn(rel, q0, n, groups, after, into=()):
                first = lax.optimization_barrier((pos, *after))[0]
                src = (own_h, far_h)[rel // 2][q0:q0 + n]
                return run_ffn(rel, q0, n, groups, cap, first, cnt, rank_in, src, [(mine, theirs)[g] for g in groups], into)

            def swap_tp(send):
                return lax.ppermute(send, 'tp', [(0, 1), (1, 0)])

            def reduce(send, keep):
                got = swap_tp(send)
                return (keep.astype(jnp.float32) + got.astype(jnp.float32)).astype(jnp.bfloat16)

            def mix(q, own, far):
                piece = run_mix(q, pos, cnt, rank_own[q], ids_own[q], gates[q], tokens, own, far)
                pieces.append((piece, lax.ppermute(piece, 'tp', [(0, 1), (1, 0)])))

            a = ffn(0, 0, 4, (0,), ())
            send, keep = a[:4], a[4:]
            a0 = ffn(0, 0, 2, (1,), a[:1], (*send[:2], *keep[:2]))
            own = [reduce(a0[i], a0[2 + i]) for i in range(2)]
            a1 = ffn(0, 2, 2, (1,), a0[:1], (*send[2:], *keep[2:]))
            own += [reduce(a1[i], a1[2 + i]) for i in range(2)]
            b0 = ffn(2, 0, 2, (0, 1), a1[:1])
            far = [reduce(b0[i], b0[2 + i]) for i in range(2)]
            b1 = ffn(2, 2, 2, (0, 1), b0[:1])
            late = [swap_tp(b1[i]) for i in range(2)]
            back = [lax.ppermute(rows, 'ep', swap_x) for rows in far]
            for i in range(2):
                mix(i, own[i], back[i])
                keep, got, _ = lax.optimization_barrier((b1[2 + i], late[i], pieces[i][0]))
                back.append(lax.ppermute((keep.astype(jnp.float32) + got.astype(jnp.float32)).astype(jnp.bfloat16), 'ep', swap_x))
            for q in range(2, 4):
                mix(q, own[q], back[q])
            for q, (piece, other) in enumerate(pieces):
                out = lax.dynamic_update_slice(out, piece, (q * quarter + half * PIECE, 0))
                out = lax.dynamic_update_slice(out, other, (q * quarter + (1 - half) * PIECE, 0))
            return out

        def own_half(v):
            return lax.dynamic_index_in_dim(v.reshape(4, 2, PIECE, -1), half, 1, keepdims=False)

        args = (tokens, own_h, pos, cnt, rank_in, own_half(rank_own), own_half(expert_ids), own_half(gates), w_gate, w_up, w_down)
        tier = run_tier(cnt, TIERS)

        def branch(i, *a):
            return body(TIERS[i], *a)

        return lax.switch(tier[0], [functools.partial(branch, i) for i in range(len(TIERS))], *args)

    return jax.shard_map(local_block, mesh=mesh, in_specs=(tok_spec, tok_spec, P(None), P(None, None), P('ep', None, 'tp'), P('ep', None, 'tp'), P('ep', 'tp', None)), out_specs=tok_spec, check_vma=False)
```
